8 devices in a mesh: rep: 1 (over z), kv: 8 (over y, x, core).
Axes of the slice: x: 2, y: 2, z: 1, core: 2. Of those that a mesh axis runs over, the one named last changes fastest.
Arguments:
- embeds: bfloat16 [2, 192, 4096], P(None, ('rep', 'kv'))
- w_query: bfloat16 [2, 4096, 4096], replicated
- w_key: bfloat16 [2, 4096, 1024], replicated
- w_value: bfloat16 [2, 4096, 1024], replicated
- w_out: bfloat16 [2, 4096, 4096], replicated
- w_up: bfloat16 [2, 4096, 14336], replicated
- w_down: bfloat16 [2, 14336, 4096], replicated
- k_pool: bfloat16 [1152, 2, 32, 8, 128], P(('rep', 'kv'))
- v_pool: bfloat16 [1152, 2, 32, 8, 128], P(('rep', 'kv'))
- old_table: int32 [192, 4], P('rep')
- new_table: int32 [192, 4], P('rep')
- seq_len: int32 [192], P('rep')
- finished: int32 [192], P('rep')
- mig_src: int32 [384], P('rep')
- mig_dst: int32 [384], P('rep')
Outputs:
- output 1: bfloat16 [2, 192, 4096], P(None, ('rep', 'kv'))
- output 2: bfloat16 [1152, 2, 32, 8, 128], P(('rep', 'kv'))
- output 3: bfloat16 [1152, 2, 32, 8, 128], P(('rep', 'kv'))
All inputs are finite; a program needn't handle non-finite values.
Results may differ from the reference program's by a relative error of at most 0.0164136.
Values are sent between devices in bfloat16 or wider.
A program may use at most 2.75 GiB of HBM per device.

```python
import jax
import jax.numpy as jnp
from jax import lax

D_MODEL = 4096
Q_HEADS = 32
KV_HEADS = 8
HEAD_DIM = 128
FF_DIM = 14336
PAGE_SIZE = 32
SEQ_DEV = 24
PAGES_SEQ = 4
PAIR_CAP = 24
GROUP_DEVS = 8
N_LAYERS = 2

Q_WIDTH = Q_HEADS * HEAD_DIM
KV_WIDTH = KV_HEADS * HEAD_DIM
HALF_DEVS = GROUP_DEVS // 2
N_BATCH = GROUP_DEVS * SEQ_DEV
DONE_SEQS = N_BATCH // 4
SLOTS_DEV = 3 * SEQ_DEV * PAGES_SEQ // 2
TOTAL_SLOTS = GROUP_DEVS * SLOTS_DEV
COLD_PAGES = PAGES_SEQ // 4
HOT_PAGES = PAGES_SEQ - COLD_PAGES
PER_DEV = N_BATCH // HALF_DEVS
DONE_PER = DONE_SEQS // HALF_DEVS
ACTIVE_PER = PER_DEV - DONE_PER
DONE_COLD = COLD_PAGES * DONE_PER
N_MIG = HALF_DEVS * HALF_DEVS * PAIR_CAP
CONTEXT = PAGES_SEQ * PAGE_SIZE


def slot_order(one_key):
    return jax.random.permutation(one_key, SLOTS_DEV)


def draw_layout(layout_key):
    key_list = jax.random.split(layout_key, 5)
    dev_perm = jax.random.permutation(key_list[0], GROUP_DEVS)
    seq_perm = jax.random.permutation(key_list[1], N_BATCH)
    slot_perm = jax.vmap(slot_order)(jax.random.split(key_list[2], GROUP_DEVS))
    entry_perm = jax.random.permutation(key_list[3], N_MIG)
    hot_devs = dev_perm[:HALF_DEVS]
    cold_devs = dev_perm[HALF_DEVS:]
    seq_ids = jnp.arange(N_BATCH)[:, None]
    page_ids = jnp.arange(PAGES_SEQ)[None, :]
    is_cold = page_ids < COLD_PAGES
    page_level = jnp.where(is_cold, page_ids, page_ids - COLD_PAGES)
    dev_pos = (seq_ids + page_level) % HALF_DEVS
    device = jnp.where(is_cold, cold_devs[dev_pos], hot_devs[dev_pos])
    slot_rank = page_level * PER_DEV + seq_ids // HALF_DEVS
    slot_ids = device * SLOTS_DEV + slot_perm[device, slot_rank]
    entry_ids = jnp.arange(N_MIG)
    src_pos = entry_ids // (HALF_DEVS * PAIR_CAP)
    dst_pos = (entry_ids // PAIR_CAP) % HALF_DEVS
    within = entry_ids % PAIR_CAP
    src_rank = dst_pos * PAIR_CAP + within
    dst_rank = src_pos * PAIR_CAP + within
    hot_level = HOT_PAGES - 1 - src_rank // ACTIVE_PER
    src_seq = DONE_SEQS + (src_pos - hot_level) % HALF_DEVS + HALF_DEVS * (src_rank % ACTIVE_PER)
    src_page = COLD_PAGES + hot_level
    src_slot = slot_ids[src_seq, src_page]
    cold_level = jnp.minimum(dst_rank // DONE_PER, COLD_PAGES - 1)
    done_seq = (dst_pos - cold_level) % HALF_DEVS + HALF_DEVS * (dst_rank % DONE_PER)
    reuse_slot = slot_ids[done_seq, cold_level]
    cold_dev = cold_devs[dst_pos]
    free_rank = jnp.clip(COLD_PAGES * PER_DEV + dst_rank - DONE_COLD, 0, SLOTS_DEV - 1)
    free_slot = cold_dev * SLOTS_DEV + slot_perm[cold_dev, free_rank]
    dst_slot = jnp.where(dst_rank < DONE_COLD, reuse_slot, free_slot)
    new_ids = slot_ids.at[src_seq, src_page].set(dst_slot)
    done_flag = (jnp.arange(N_BATCH) < DONE_SEQS).astype(jnp.int32)
    seq_len = jax.random.randint(key_list[4], (N_BATCH,), (PAGES_SEQ - 1) * PAGE_SIZE, CONTEXT - 1)
    seq_len = seq_len.at[seq_perm[N_BATCH - 1]].set(CONTEXT - 2)
    seq_len = seq_len.at[seq_perm[N_BATCH - 2]].set((PAGES_SEQ - 1) * PAGE_SIZE)
    blank_table = jnp.zeros((N_BATCH, PAGES_SEQ), jnp.int32)
    return {
        'old_table': blank_table.at[seq_perm].set(slot_ids.astype(jnp.int32)),
        'new_table': blank_table.at[seq_perm].set(new_ids.astype(jnp.int32)),
        'seq_len': seq_len.astype(jnp.int32),
        'finished': jnp.zeros((N_BATCH,), jnp.int32).at[seq_perm].set(done_flag),
        'mig_src': jnp.zeros((N_MIG,), jnp.int32).at[entry_perm].set(src_slot.astype(jnp.int32)),
        'mig_dst': jnp.zeros((N_MIG,), jnp.int32).at[entry_perm].set(dst_slot.astype(jnp.int32)),
    }


def draw_weight(one_key, fan_in, fan_out, gain):
    values = jax.random.normal(one_key, (N_LAYERS, fan_in, fan_out), jnp.float32)
    return (values * (gain * fan_in ** -0.5)).astype(jnp.bfloat16)


def setup_inputs(seed: int = 0, part: int = 0) -> dict:
    shared = jax.random.split(jax.random.key(seed), 6)
    part_keys = jax.random.split(jax.random.fold_in(jax.random.key(seed + 1), part), 5)
    layout = draw_layout(part_keys[0])
    pool_shape = (TOTAL_SLOTS, N_LAYERS, PAGE_SIZE, KV_HEADS, HEAD_DIM)
    page_mean = jax.random.normal(part_keys[3], (TOTAL_SLOTS, N_LAYERS, 1, KV_HEADS, HEAD_DIM), jnp.float32)
    v_noise = jax.random.normal(part_keys[4], pool_shape, jnp.float32)
    return {
        'embeds': jax.random.normal(part_keys[1], (2, N_BATCH, D_MODEL), jnp.float32).astype(jnp.bfloat16),
        'w_query': draw_weight(shared[0], D_MODEL, Q_WIDTH, 1.0),
        'w_key': draw_weight(shared[1], D_MODEL, KV_WIDTH, 1.0),
        'w_value': draw_weight(shared[2], D_MODEL, KV_WIDTH, 1.0),
        'w_out': draw_weight(shared[3], Q_WIDTH, D_MODEL, (0.5 * PAGES_SEQ) ** 0.5),
        'w_up': draw_weight(shared[4], D_MODEL, FF_DIM, 1.0),
        'w_down': draw_weight(shared[5], FF_DIM, D_MODEL, 1.0),
        'k_pool': jax.random.normal(part_keys[2], pool_shape, jnp.float32).astype(jnp.bfloat16),
        'v_pool': (page_mean + 0.5 * v_noise).astype(jnp.bfloat16),
        'old_table': layout['old_table'],
        'new_table': layout['new_table'],
        'seq_len': layout['seq_len'],
        'finished': layout['finished'],
        'mig_src': layout['mig_src'],
        'mig_dst': layout['mig_dst'],
    }


def project(hidden, w_mat):
    return jnp.dot(hidden, w_mat, preferred_element_type=jnp.float32).astype(jnp.bfloat16)


def attend(query_rows, k_layer, v_layer, table, lengths):
    def one_seq(operands):
        q_row, table_row, length = operands
        page_keys = k_layer[table_row].astype(jnp.float32).reshape(CONTEXT, KV_HEADS, HEAD_DIM)
        page_vals = v_layer[table_row].astype(jnp.float32).reshape(CONTEXT, KV_HEADS, HEAD_DIM)
        q_grouped = q_row.astype(jnp.float32).reshape(KV_HEADS, Q_HEADS // KV_HEADS, HEAD_DIM)
        scores = jnp.einsum('grd,tgd->grt', q_grouped, page_keys) * (HEAD_DIM ** -0.5)
        valid_pos = jnp.arange(CONTEXT) <= length
        scores = jnp.where(valid_pos, scores, -jnp.inf)
        weights = jax.nn.softmax(scores, axis=-1)
        mixed = jnp.einsum('grt,tgd->grd', weights, page_vals)
        return mixed.reshape(Q_WIDTH).astype(jnp.bfloat16)
    return lax.map(one_seq, (query_rows, table, lengths))


def finish_block(hidden, attn_rows, w_out, w_up, w_down):
    mixed_rows = (hidden.astype(jnp.float32) + jnp.dot(attn_rows, w_out, preferred_element_type=jnp.float32)).astype(jnp.bfloat16)
    inner_act = jax.nn.gelu(jnp.dot(mixed_rows, w_up, preferred_element_type=jnp.float32)).astype(jnp.bfloat16)
    return (mixed_rows.astype(jnp.float32) + jnp.dot(inner_act, w_down, preferred_element_type=jnp.float32)).astype(jnp.bfloat16)


def reference(embeds, w_query, w_key, w_value, w_out, w_up, w_down, k_pool, v_pool, old_table, new_table, seq_len, finished, mig_src, mig_dst):
    seq_ids = jnp.arange(N_BATCH)
    active = finished == 0
    len_next = seq_len + 1
    slot_zero = old_table[seq_ids, seq_len // PAGE_SIZE]
    slot_one = jnp.where(active, new_table[seq_ids, len_next // PAGE_SIZE], TOTAL_SLOTS)
    hid_zero = embeds[0]
    hid_one = embeds[1]
    k_layers = []
    v_layers = []
    for layer_idx in range(N_LAYERS):
        k_layer = k_pool[:, layer_idx]
        v_layer = v_pool[:, layer_idx]
        query_rows = project(hid_zero, w_query[layer_idx])
        k_new = project(hid_zero, w_key[layer_idx]).reshape(N_BATCH, KV_HEADS, HEAD_DIM)
        v_new = project(hid_zero, w_value[layer_idx]).reshape(N_BATCH, KV_HEADS, HEAD_DIM)
        k_layer = k_layer.at[slot_zero, seq_len % PAGE_SIZE].set(k_new)
        v_layer = v_layer.at[slot_zero, seq_len % PAGE_SIZE].set(v_new)
        attn_rows = attend(query_rows, k_layer, v_layer, old_table, seq_len)
        hid_zero = finish_block(hid_zero, attn_rows, w_out[layer_idx], w_up[layer_idx], w_down[layer_idx])
        k_layer = k_layer.at[mig_dst].set(k_layer[mig_src])
        v_layer = v_layer.at[mig_dst].set(v_layer[mig_src])
        query_rows = project(hid_one, w_query[layer_idx])
        k_new = project(hid_one, w_key[layer_idx]).reshape(N_BATCH, KV_HEADS, HEAD_DIM)
        v_new = project(hid_one, w_value[layer_idx]).reshape(N_BATCH, KV_HEADS, HEAD_DIM)
        k_layer = k_layer.at[slot_one, len_next % PAGE_SIZE].set(k_new, mode='drop')
        v_layer = v_layer.at[slot_one, len_next % PAGE_SIZE].set(v_new, mode='drop')
        attn_rows = attend(query_rows, k_layer, v_layer, new_table, len_next)
        hid_one = finish_block(hid_one, attn_rows, w_out[layer_idx], w_up[layer_idx], w_down[layer_idx])
        k_layers.append(k_layer)
        v_layers.append(v_layer)
    hid_one = jnp.where(active[:, None], hid_one, jnp.zeros_like(hid_one))
    return jnp.stack([hid_zero, hid_one]), jnp.stack(k_layers, axis=1), jnp.stack(v_layers, axis=1)
```

```python
import functools

import jax
import jax.numpy as jnp
from jax import lax
from jax.experimental import pallas as pl
from jax.experimental.pallas import tpu as pltpu
from jax.sharding import PartitionSpec as P


MESH = pl.DeviceIdType.MESH
ANY = pl.BlockSpec(memory_space=pl.ANY)
VMEM = pl.BlockSpec(memory_space=pltpu.VMEM)
SMEM = pl.BlockSpec(memory_space=pltpu.SMEM)
NEG = -3e38
ENTRY_PAD = 160
GROUP = 4
DEPTH = 6
RING = 16
LAG = 8
CHUNKS = ((0, 0, 3), (0, 3, 13), (0, 13, 24), (1, 0, 16), (1, 16, 24))


def peers():
    rep = lax.axis_index('rep')
    me = lax.axis_index('kv')
    core = lax.rem(me, 2)
    chip = me // 2
    x = lax.rem(chip, 2)
    y = chip // 2
    partner = me + 1 - 2 * core
    chips = (y * 2 + (1 - x), (1 - y) * 2 + x, (1 - y) * 2 + (1 - x))
    return rep, me, core, chip, partner, chips


def meet(rep, others):
    barrier = pltpu.get_barrier_semaphore()
    for other in others:
        pl.semaphore_signal(barrier, inc=1, device_id=(rep, other), device_id_type=MESH)
    pl.semaphore_wait(barrier, len(others))


def gather_kernel(x_ref, out_ref, local_sem, send_sems, recv_sems):
    rep, me, core, _, partner, chips = peers()
    same = [c * 2 + core for c in chips]
    meet(rep, same + [partner])
    own = pltpu.make_async_copy(x_ref, out_ref.at[me], local_sem)

    def remote(src, dst_at, k, dev):
        return pltpu.make_async_remote_copy(src_ref=src, dst_ref=out_ref.at[dst_at], send_sem=send_sems.at[k], recv_sem=recv_sems.at[k], device_id=(rep, dev), device_id_type=MESH)

    across = [remote(x_ref, me, k, same[k]) for k in (2, 0, 1)]
    for copy in across:
        copy.start()
    to_partner = remote(x_ref, me, 3, partner)
    to_partner.start()
    own.start()
    forwards = []
    for k in (0, 1, 2):
        remote(x_ref, me, k, same[k]).wait_recv()
        forward = remote(out_ref.at[same[k]], same[k], 4 + k, partner)
        forward.start()
        forwards.append(forward)
    own.wait()
    for copy in across:
        copy.wait_send()
    to_partner.wait()
    for forward in forwards:
        forward.wait()


def gather_rows(x, collective_id, groups):
    return pl.pallas_call(
        gather_kernel,
        out_shape=jax.ShapeDtypeStruct((groups,) + x.shape, x.dtype),
        in_specs=[VMEM],
        out_specs=ANY,
        scratch_shapes=[pltpu.SemaphoreType.DMA, pltpu.SemaphoreType.DMA((7,)), pltpu.SemaphoreType.DMA((7,))],
        compiler_params=pltpu.CompilerParams(collective_id=collective_id, has_side_effects=True),
        name='gather_rows',
    )(x)


def swap_kernel(o_ref, s_ref, o_out, s_out, send_sems, recv_sems):
    rep, _, core, _, partner, _ = peers()
    meet(rep, [partner])
    copies = []
    for c in range(4):
        theirs = c * 2 + (1 - core)
        copies.append(pltpu.make_async_remote_copy(src_ref=o_ref.at[theirs], dst_ref=o_out.at[c], send_sem=send_sems.at[c], recv_sem=recv_sems.at[c], device_id=(rep, partner), device_id_type=MESH))
        copies.append(pltpu.make_async_remote_copy(src_ref=s_ref.at[theirs], dst_ref=s_out.at[c], send_sem=send_sems.at[4 + c], recv_sem=recv_sems.at[4 + c], device_id=(rep, partner), device_id_type=MESH))
    for copy in copies:
        copy.start()
    for copy in copies:
        copy.wait()


def swap_partials(o, s, collective_id):
    return pl.pallas_call(
        swap_kernel,
        out_shape=(jax.ShapeDtypeStruct((4,) + o.shape[1:], o.dtype), jax.ShapeDtypeStruct((4,) + s.shape[1:], s.dtype)),
        in_specs=[ANY, ANY],
        out_specs=(ANY, ANY),
        scratch_shapes=[pltpu.SemaphoreType.DMA((8,)), pltpu.SemaphoreType.DMA((8,))],
        compiler_params=pltpu.CompilerParams(collective_id=collective_id, has_side_effects=True),
        name='swap_partials',
    )(o, s)


def home_kernel(o_ref, s_ref, o_out, s_out, send_sems, recv_sems):
    rep, _, core, _, _, chips = peers()
    same = [c * 2 + core for c in chips]
    meet(rep, same)
    copies = []
    for k in (2, 0, 1):
        copies.append(pltpu.make_async_remote_copy(src_ref=o_ref.at[chips[k]], dst_ref=o_out.at[k], send_sem=send_sems.at[k], recv_sem=recv_sems.at[k], device_id=(rep, same[k]), device_id_type=MESH))
        copies.append(pltpu.make_async_remote_copy(src_ref=s_ref.at[chips[k]], dst_ref=s_out.at[k], send_sem=send_sems.at[3 + k], recv_sem=recv_sems.at[3 + k], device_id=(rep, same[k]), device_id_type=MESH))
    for copy in copies:
        copy.start()
    for copy in copies:
        copy.wait()


def home_partials(o, s, collective_id):
    return pl.pallas_call(
        home_kernel,
        out_shape=(jax.ShapeDtypeStruct((3,) + o.shape[1:], o.dtype), jax.ShapeDtypeStruct((3,) + s.shape[1:], s.dtype)),
        in_specs=[ANY, ANY],
        out_specs=(ANY, ANY),
        scratch_shapes=[pltpu.SemaphoreType.DMA((6,)), pltpu.SemaphoreType.DMA((6,))],
        compiler_params=pltpu.CompilerParams(collective_id=collective_id, has_side_effects=True),
        name='home_partials',
    )(o, s)


def attend_kernel(layer, n_seq, heads, scale, list_ref, q_ref, k_hbm, v_hbm, o_ref, m_out, l_out, m_acc, l_acc, kbuf, vbuf, sems):
    rows, dim = q_ref.shape[1:]
    keys = kbuf.shape[2]
    n_groups = (list_ref[3, 0] + GROUP - 1) // GROUP

    def copies(g, buf):
        out = []
        for j in range(GROUP):
            slot = list_ref[1, g * GROUP + j]
            out.append(pltpu.make_async_copy(k_hbm.at[slot, layer], kbuf.at[buf, j], sems.at[buf]))
            out.append(pltpu.make_async_copy(v_hbm.at[slot, layer], vbuf.at[buf, j], sems.at[buf]))
        return out

    for g in range(DEPTH):
        @pl.when(g < n_groups)
        def _():
            for copy in copies(g, g):
                copy.start()

    def clear(i, carry):
        o_ref[i] = jnp.zeros((rows, dim), jnp.float32)
        m_acc[i] = jnp.full((rows, dim), NEG, jnp.float32)
        l_acc[i] = jnp.zeros((rows, dim), jnp.float32)
        return carry

    lax.fori_loop(0, n_seq, clear, 0)

    row = lax.broadcasted_iota(jnp.int32, (rows, keys), 0)
    col = lax.broadcasted_iota(jnp.int32, (rows, keys), 1)
    same_head = lax.rem(col, heads) == lax.rem(row, rows // 2) // (rows // 2 // heads)
    position = jnp.where(same_head, col // heads, keys)

    def group(g, carry):
        buf = lax.rem(g, DEPTH)
        for copy in copies(g, buf):
            copy.wait()
        parts = []
        for j in range(GROUP):
            e = g * GROUP + j
            seq = list_ref[0, e]
            mask = position < list_ref[2, e]
            scores = lax.dot_general(q_ref[seq], kbuf[buf, j], (((1,), (1,)), ((), ())), preferred_element_type=jnp.float32) * scale
            scores = jnp.where(mask, scores, NEG)
            top = jnp.max(scores, axis=1, keepdims=True)
            weights = jnp.where(mask, jnp.exp(scores - top), 0.0)
            total = jnp.sum(weights, axis=1, keepdims=True)
            mixed = jnp.dot(weights.astype(jnp.bfloat16), vbuf[buf, j], preferred_element_type=jnp.float32)
            parts.append((seq, top, total, mixed))
        for seq, top, total, mixed in parts:
            top_old = m_acc[seq]
            top_new = jnp.maximum(top_old, top)
            keep = jnp.exp(top_old - top_new)
            add = jnp.exp(top - top_new)
            m_acc[seq] = top_new
            l_acc[seq] = l_acc[seq] * keep + total * add
            o_ref[seq] = o_ref[seq] * keep + mixed * add

        @pl.when(g + DEPTH < n_groups)
        def _():
            for copy in copies(g + DEPTH, buf):
                copy.start()

        return carry

    lax.fori_loop(0, n_groups, group, 0)

    lane = lax.broadcasted_iota(jnp.int32, (rows, dim), 1)
    for part in range(2):
        first = part * dim
        many = min(dim, n_seq - first)

        def pack(i, carry):
            tops, totals = carry
            here = lane == i
            return jnp.where(here, m_acc[first + i], tops), jnp.where(here, l_acc[first + i], totals)

        zero = jnp.zeros((rows, dim), jnp.float32)
        tops, totals = lax.fori_loop(0, many, pack, (zero, zero))
        m_out[:, first:first + dim] = tops
        l_out[:, first:first + dim] = totals


def attend_pages(lists, q_all, k_pool, v_pool, layer, heads, scale):
    n_seq, rows, dim = q_all.shape
    keys = k_pool.shape[2]
    return pl.pallas_call(
        functools.partial(attend_kernel, layer, n_seq, heads, scale),
        out_shape=(
            jax.ShapeDtypeStruct((n_seq, rows, dim), jnp.float32),
            jax.ShapeDtypeStruct((rows, 2 * dim), jnp.float32),
            jax.ShapeDtypeStruct((rows, 2 * dim), jnp.float32),
        ),
        in_specs=[SMEM, VMEM, ANY, ANY],
        out_specs=(VMEM, VMEM, VMEM),
        scratch_shapes=[
            pltpu.VMEM((n_seq, rows, dim), jnp.float32),
            pltpu.VMEM((n_seq, rows, dim), jnp.float32),
            pltpu.VMEM((DEPTH, GROUP, keys, dim), k_pool.dtype),
            pltpu.VMEM((DEPTH, GROUP, keys, dim), v_pool.dtype),
            pltpu.SemaphoreType.DMA((DEPTH,)),
        ],
        compiler_params=pltpu.CompilerParams(vmem_limit_bytes=48 * 1024 * 1024),
        cost_estimate=pl.CostEstimate(flops=40_000_000_000, bytes_accessed=30_000_000, transcendentals=0),
        name='attend_pages',
    )(lists, q_all, k_pool, v_pool)


def patch_kernel(list_ref, rows_ref, k_in, v_in, k_out, v_out, sem):
    many = list_ref[3, 0]

    def copies(i):
        row, slot, offset = list_ref[0, i], list_ref[1, i], list_ref[2, i]
        return [pltpu.make_async_copy(rows_ref.at[row, kind], ref.at[slot, :, offset], sem) for kind, ref in ((0, k_out), (1, v_out))]

    def start(i, carry):
        for copy in copies(i):
            copy.start()
        return carry

    def finish(i, carry):
        for copy in copies(i):
            copy.wait()
        return carry

    lax.fori_loop(0, many, start, 0)
    lax.fori_loop(0, many, finish, 0)


def patch_pools(writes, rows, k_pool, v_pool):
    return pl.pallas_call(
        patch_kernel,
        out_shape=(jax.ShapeDtypeStruct(k_pool.shape, k_pool.dtype), jax.ShapeDtypeStruct(v_pool.shape, v_pool.dtype)),
        in_specs=[SMEM, VMEM, ANY, ANY],
        out_specs=(ANY, ANY),
        scratch_shapes=[pltpu.SemaphoreType.DMA],
        input_output_aliases={2: 0, 3: 1},
        name='patch_pools',
    )(writes, rows, k_pool, v_pool)


def move_kernel(list_ref, src_ref, *refs):
    dst_ref, ring, in_sems, out_sems = refs[-4:]
    many = list_ref[2, 0]

    def fetch(i):
        buf = lax.rem(i, RING)
        return pltpu.make_async_copy(src_ref.at[list_ref[0, i]], ring.at[buf], in_sems.at[buf])

    def store(i):
        buf = lax.rem(i, RING)
        return pltpu.make_async_copy(ring.at[buf], dst_ref.at[list_ref[1, i]], out_sems.at[buf])

    def first(i, carry):
        fetch(i).start()
        return carry

    def step(i, carry):
        fetch(i).wait()
        store(i).start()

        @pl.when(i >= LAG)
        def _():
            store(i - LAG).wait()

            @pl.when(i - LAG + RING < many)
            def _():
                fetch(i - LAG + RING).start()

        return carry

    def last(i, carry):
        store(i).wait()
        return carry

    lax.fori_loop(0, jnp.minimum(many, RING), first, 0)
    lax.fori_loop(0, many, step, 0)
    lax.fori_loop(jnp.maximum(many - LAG, 0), many, last, 0)


def move_pages(moves, src, dst):
    fresh = isinstance(dst, tuple)
    shape = dst if fresh else dst.shape
    return pl.pallas_call(
        move_kernel,
        out_shape=jax.ShapeDtypeStruct(shape, src.dtype),
        in_specs=[SMEM, ANY] if fresh else [SMEM, ANY, ANY],
        out_specs=ANY,
        scratch_shapes=[pltpu.VMEM((RING,) + src.shape[1:], src.dtype), pltpu.SemaphoreType.DMA((RING,)), pltpu.SemaphoreType.DMA((RING,))],
        input_output_aliases={} if fresh else {2: 0},
    )(*((moves, src) if fresh else (moves, src, dst)))


def compact(keep, size, *columns):
    n = keep.shape[-1]
    place = jnp.arange(n, dtype=jnp.int32)
    before = (place[:, None] < place[None, :]).astype(jnp.bfloat16)
    rank = jnp.dot(keep.astype(jnp.bfloat16), before, preferred_element_type=jnp.float32).astype(jnp.int32)
    rank = jnp.where(keep, rank, -1)
    hit = rank[:, None, :] == jnp.arange(size, dtype=jnp.int32)[None, :, None]
    packed = [jnp.sum(jnp.where(hit, column[:, None, :], 0), axis=-1) for column in columns]
    many = jnp.sum(keep.astype(jnp.int32), axis=-1)
    return jnp.stack(packed + [jnp.broadcast_to(many[:, None], packed[0].shape)], axis=1)


def solution(mesh):
    groups = mesh.shape['kv']
    rows_spec = P(None, ('rep', 'kv'), None)
    pool_spec = P(('rep', 'kv'))
    table_spec = P('rep', None)
    vec_spec = P('rep')
    full_spec = P()

    def device_fn(embeds, w_query, w_key, w_value, w_out, w_up, w_down, k_pool, v_pool, old_table, new_table, seq_len, finished, mig_src, mig_dst):
        my_dev = lax.axis_index('kv')
        slots_dev, n_layers, page_size, kv_heads, head_dim = k_pool.shape
        n_steps, seq_dev, d_model = embeds.shape
        n_batch, pages_seq = old_table.shape
        q_width = w_query.shape[2]
        kv_width = kv_heads * head_dim
        rep_factor = q_width // kv_width
        q_heads = kv_heads * rep_factor
        n_mig = mig_src.shape[0]
        scale = head_dim ** -0.5
        slot_base = my_dev * slots_dev
        last_page = pages_seq - 1
        active = finished == 0

        src_dev = mig_src // slots_dev
        dst_dev = mig_dst // slots_dev
        pair_key = src_dev * groups + dst_dev
        entry_ids = jnp.arange(n_mig, dtype=jnp.int32)
        earlier = (pair_key[None, :] == pair_key[:, None]) & (entry_ids[None, :] < entry_ids[:, None])
        pair_rank = jnp.sum(earlier.astype(jnp.int32), axis=1)
        keeps, froms, tos = [], [], []
        for pool, low, high in CHUNKS:
            wide = high - low
            ranked = (pair_rank >= low) & (pair_rank < high)
            keeps.append(ranked & (src_dev == my_dev))
            froms.append(mig_src - slot_base)
            tos.append(dst_dev * wide + pair_rank - low)
            keeps.append(ranked & (dst_dev == my_dev))
            froms.append(src_dev * wide + pair_rank - low)
            tos.append(mig_dst - slot_base)
        plan = compact(jnp.stack(keeps), slots_dev, jnp.stack(froms), jnp.stack(tos))
        pools = (k_pool, v_pool)
        received = [None] * len(CHUNKS)

        def pack(c, after=None):
            pool, low, high = CHUNKS[c]
            moves = plan[2 * c]
            if after is not None:
                moves, _ = lax.optimization_barrier((moves, after))
            return move_pages(moves, pools[pool], (groups * (high - low),) + k_pool.shape[1:])

        def send(c, pages, after=None):
            if after is not None:
                pages, _ = lax.optimization_barrier((pages, after))
            received[c] = lax.all_to_all(pages, 'kv', 0, 0, tiled=True)

        page_slot = old_table.reshape(-1) - slot_base
        here = (page_slot >= 0) & (page_slot < slots_dev)
        page_seq = jnp.repeat(jnp.arange(n_batch, dtype=jnp.int32), pages_seq)
        page_start = jnp.tile(jnp.arange(pages_seq, dtype=jnp.int32) * page_size, n_batch)
        page_valid = jnp.clip(jnp.repeat(seq_len, pages_seq) - page_start, 0, page_size)
        lists = compact(here[None], ENTRY_PAD, page_seq[None], page_slot[None], page_valid[None])[0]

        old_last = old_table[:, last_page]
        new_last = new_table[:, last_page]
        overwritten = jnp.any(old_last[:, None] == mig_dst[None, :], axis=1)
        moved = active & (new_last != old_last)
        seq_ids = jnp.arange(n_batch, dtype=jnp.int32)
        offset = seq_len - last_page * page_size
        write_slot = jnp.concatenate([jnp.where(overwritten, -1, old_last), jnp.where(moved, new_last, -1), jnp.where(active, new_last, -1)]) - slot_base
        write_row = jnp.concatenate([seq_ids * 2, seq_ids * 2, seq_ids * 2 + 1])
        write_offset = jnp.concatenate([offset, offset, offset + 1])
        write_here = (write_slot >= 0) & (write_slot < slots_dev)
        writes = compact(write_here[None], 2 * slots_dev, write_row[None], write_slot[None], write_offset[None])[0]

        k_pages = k_pool.reshape(slots_dev, n_layers, page_size * kv_heads, head_dim)
        v_pages = v_pool.reshape(slots_dev, n_layers, page_size * kv_heads, head_dim)
        rows = seq_dev * n_steps
        lanes = n_steps * q_heads

        def dot(a, b):
            return jnp.dot(a, b, preferred_element_type=jnp.float32)

        def split(stats):
            return stats[..., :lanes], stats[..., lanes:]

        send(0, pack(0))
        hidden = embeds.transpose(1, 0, 2).reshape(rows, d_model)
        new_rows = []
        for layer in range(n_layers):
            query = dot(hidden, w_query[layer]).astype(jnp.bfloat16).reshape(seq_dev, lanes, head_dim)
            k_new = dot(hidden, w_key[layer]).astype(jnp.bfloat16).reshape(seq_dev, n_steps, kv_heads, head_dim)
            v_new = dot(hidden, w_value[layer]).astype(jnp.bfloat16).reshape(seq_dev, n_steps, kv_heads, head_dim)
            new_rows.append(jnp.stack([k_new, v_new], axis=2))

            packed = pack(layer + 1, query)
            q_all = gather_rows(query, 3 * layer, groups).reshape(n_batch, lanes, head_dim)
            o_part, m_part, l_part = attend_pages(lists, q_all, k_pages, v_pages, layer, kv_heads, scale)
            stats = jnp.concatenate([m_part.T[:n_batch], l_part.T[:n_batch]], axis=1).reshape(groups, seq_dev, 2 * lanes)
            o_part = o_part.reshape(groups, seq_dev, lanes, head_dim)

            o_recv, s_recv = swap_partials(o_part, stats, 3 * layer + 1)
            core = lax.rem(my_dev, 2)
            chip = my_dev // 2
            o_mine = lax.dynamic_index_in_dim(o_part.reshape(groups // 2, 2, seq_dev, lanes, head_dim), core, 1, keepdims=False)
            s_mine = lax.dynamic_index_in_dim(stats.reshape(groups // 2, 2, seq_dev, 2 * lanes), core, 1, keepdims=False)
            m_a, l_a = split(s_mine)
            m_b, l_b = split(s_recv)
            m_chip = jnp.maximum(m_a, m_b)
            f_a, f_b = jnp.exp(m_a - m_chip), jnp.exp(m_b - m_chip)
            o_chip = o_mine * f_a[..., None] + o_recv * f_b[..., None]
            s_chip = jnp.concatenate([m_chip, l_a * f_a + l_b * f_b], axis=-1)

            o_far, s_far = home_partials(o_chip, s_chip, 3 * layer + 2)
            send(layer + 1, packed, o_far)
            o_near = lax.dynamic_index_in_dim(o_chip, chip, 0, keepdims=False)
            m_near, l_near = split(lax.dynamic_index_in_dim(s_chip, chip, 0, keepdims=False))
            m_far, l_far = split(s_far)
            q_own = query.astype(jnp.float32).reshape(seq_dev, n_steps, 1, kv_heads, rep_factor, head_dim)
            k_own = k_new.astype(jnp.float32).reshape(seq_dev, 1, n_steps, kv_heads, 1, head_dim)
            own = jnp.sum(q_own * k_own, axis=-1) * scale
            seen = jnp.arange(n_steps)[None, :] <= jnp.arange(n_steps)[:, None]
            own = jnp.where(seen[None, :, :, None, None], own, NEG)
            m_own = own.max(axis=2).reshape(seq_dev, lanes)
            m_all = jnp.maximum(jnp.maximum(m_near, m_far.max(axis=0)), m_own)
            p_own = jnp.exp(own - m_all.reshape(seq_dev, n_steps, 1, kv_heads, rep_factor))
            v_own = v_new.astype(jnp.float32).reshape(seq_dev, 1, n_steps, kv_heads, 1, head_dim)
            o_own = jnp.sum(p_own[..., None] * v_own, axis=2).reshape(seq_dev, lanes, head_dim)
            f_near = jnp.exp(m_near - m_all)
            f_far = jnp.exp(m_far - m_all)
            total = l_near * f_near + jnp.sum(l_far * f_far, axis=0) + jnp.sum(p_own, axis=2).reshape(seq_dev, lanes)
            o_all = o_own + o_near * f_near[..., None]
            for k in range(3):
                o_all = o_all + o_far[k] * f_far[k][..., None]
            attn = (o_all / total[..., None]).astype(jnp.bfloat16).reshape(rows, q_width)

            mixed = (hidden.astype(jnp.float32) + dot(attn, w_out[layer])).astype(jnp.bfloat16)
            inner = jax.nn.gelu(dot(mixed, w_up[layer])).astype(jnp.bfloat16)
            hidden = (mixed.astype(jnp.float32) + dot(inner, w_down[layer])).astype(jnp.bfloat16)

        rows_here = jnp.stack(new_rows, axis=3)
        rows_all = lax.all_gather(rows_here, 'kv', axis=0, tiled=True).reshape(n_batch * n_steps, 2, n_layers, kv_heads, head_dim)

        for c in range(n_layers + 1, len(CHUNKS)):
            send(c, pack(c, hidden))
        slot_ids = jnp.arange(slots_dev, dtype=jnp.int32)
        every = jnp.stack([slot_ids, slot_ids, jnp.full((slots_dev,), slots_dev, jnp.int32)])
        every, takes, _ = lax.optimization_barrier((every, plan[1::2], hidden))
        outs = [move_pages(every, pool, pool.shape) for pool in pools]
        for c, (pool, low, high) in enumerate(CHUNKS):
            outs[pool] = move_pages(takes[c], received[c], outs[pool])
        k_out, v_out = patch_pools(writes, rows_all, *outs)

        home_done = lax.dynamic_slice(finished, (my_dev * seq_dev,), (seq_dev,))
        hidden = hidden.reshape(seq_dev, n_steps, d_model)
        hid_one = jnp.where(home_done[:, None] == 0, hidden[:, 1], jnp.zeros_like(hidden[:, 1]))
        return jnp.stack([hidden[:, 0], hid_one]), k_out, v_out

    in_specs = (rows_spec, full_spec, full_spec, full_spec, full_spec, full_spec, full_spec, pool_spec, pool_spec, table_spec, table_spec, vec_spec, vec_spec, vec_spec, vec_spec)

    return jax.shard_map(device_fn, mesh=mesh, in_specs=in_specs, out_specs=(rows_spec, pool_spec, pool_spec), check_vma=False)
```

```python
import functools

import jax
import jax.numpy as jnp
from jax import lax
from jax.experimental import pallas as pl
from jax.experimental.pallas import tpu as pltpu
from jax.sharding import PartitionSpec as P


MESH = pl.DeviceIdType.MESH
ANY = pl.BlockSpec(memory_space=pl.ANY)
VMEM = pl.BlockSpec(memory_space=pltpu.VMEM)
SMEM = pl.BlockSpec(memory_space=pltpu.SMEM)
NEG = -3e38
ENTRY_PAD = 160
GROUP = 4
DEPTH = 6
RING = 16
LAG = 8
CHUNKS = ((0, 0, 3), (0, 3, 10), (0, 10, 24), (1, 0, 6), (1, 6, 16), (1, 16, 24))


def peers():
    rep = lax.axis_index('rep')
    me = lax.axis_index('kv')
    core = lax.rem(me, 2)
    chip = me // 2
    x = lax.rem(chip, 2)
    y = chip // 2
    partner = me + 1 - 2 * core
    chips = (y * 2 + (1 - x), (1 - y) * 2 + x, (1 - y) * 2 + (1 - x))
    return rep, me, core, chip, partner, chips


def meet(rep, others):
    barrier = pltpu.get_barrier_semaphore()
    for other in others:
        pl.semaphore_signal(barrier, inc=1, device_id=(rep, other), device_id_type=MESH)
    pl.semaphore_wait(barrier, len(others))


def gather_kernel(many, *refs):
    x_refs, out_refs = refs[:many], refs[many:2 * many]
    local_sems, send_sems, recv_sems = refs[2 * many:]
    rep, me, core, _, partner, chips = peers()
    same = [c * 2 + core for c in chips]
    meet(rep, same + [partner])

    def remote(a, src, dst_at, k, dev):
        return pltpu.make_async_remote_copy(src_ref=src, dst_ref=out_refs[a].at[dst_at], send_sem=send_sems.at[a, k], recv_sem=recv_sems.at[a, k], device_id=(rep, dev), device_id_type=MESH)

    across = [remote(a, x_refs[a], me, k, same[k]) for a in range(many) for k in (2, 0, 1)]
    to_partner = [remote(a, x_refs[a], me, 3, partner) for a in range(many)]
    own = [pltpu.make_async_copy(x_refs[a], out_refs[a].at[me], local_sems.at[a]) for a in range(many)]
    for copy in across + to_partner + own:
        copy.start()
    forwards = []
    for a in range(many):
        for k in (2, 0, 1):
            remote(a, x_refs[a], me, k, same[k]).wait_recv()
            forward = remote(a, out_refs[a].at[same[k]], same[k], 4 + k, partner)
            forward.start()
            forwards.append(forward)
    for copy in own:
        copy.wait()
    for copy in across:
        copy.wait_send()
    for copy in to_partner + forwards:
        copy.wait()


def gather_rows(arrays, collective_id, groups):
    many = len(arrays)
    return pl.pallas_call(
        functools.partial(gather_kernel, many),
        out_shape=tuple(jax.ShapeDtypeStruct((groups,) + x.shape, x.dtype) for x in arrays),
        in_specs=[VMEM] * many,
        out_specs=(ANY,) * many,
        scratch_shapes=[pltpu.SemaphoreType.DMA((many,)), pltpu.SemaphoreType.DMA((many, 7)), pltpu.SemaphoreType.DMA((many, 7))],
        compiler_params=pltpu.CompilerParams(collective_id=collective_id, has_side_effects=True),
        name='gather_rows',
    )(*arrays)


def swap_kernel(o_ref, s_ref, o_out, s_out, send_sems, recv_sems):
    rep, _, core, _, partner, _ = peers()
    meet(rep, [partner])
    copies = []
    for c in range(4):
        theirs = c * 2 + (1 - core)
        copies.append(pltpu.make_async_remote_copy(src_ref=o_ref.at[theirs], dst_ref=o_out.at[c], send_sem=send_sems.at[c], recv_sem=recv_sems.at[c], device_id=(rep, partner), device_id_type=MESH))
        copies.append(pltpu.make_async_remote_copy(src_ref=s_ref.at[theirs], dst_ref=s_out.at[c], send_sem=send_sems.at[4 + c], recv_sem=recv_sems.at[4 + c], device_id=(rep, partner), device_id_type=MESH))
    for copy in copies:
        copy.start()
    for copy in copies:
        copy.wait()


def swap_partials(o, s, collective_id):
    return pl.pallas_call(
        swap_kernel,
        out_shape=(jax.ShapeDtypeStruct((4,) + o.shape[1:], o.dtype), jax.ShapeDtypeStruct((4,) + s.shape[1:], s.dtype)),
        in_specs=[ANY, ANY],
        out_specs=(ANY, ANY),
        scratch_shapes=[pltpu.SemaphoreType.DMA((8,)), pltpu.SemaphoreType.DMA((8,))],
        compiler_params=pltpu.CompilerParams(collective_id=collective_id, has_side_effects=True),
        name='swap_partials',
    )(o, s)


def home_kernel(o_ref, s_ref, o_out, s_out, send_sems, recv_sems):
    rep, _, core, _, _, chips = peers()
    same = [c * 2 + core for c in chips]
    meet(rep, same)
    copies = []
    for k in (2, 0, 1):
        copies.append(pltpu.make_async_remote_copy(src_ref=o_ref.at[chips[k]], dst_ref=o_out.at[k], send_sem=send_sems.at[k], recv_sem=recv_sems.at[k], device_id=(rep, same[k]), device_id_type=MESH))
        copies.append(pltpu.make_async_remote_copy(src_ref=s_ref.at[chips[k]], dst_ref=s_out.at[k], send_sem=send_sems.at[3 + k], recv_sem=recv_sems.at[3 + k], device_id=(rep, same[k]), device_id_type=MESH))
    for copy in copies:
        copy.start()
    for copy in copies:
        copy.wait()


def home_partials(o, s, collective_id):
    return pl.pallas_call(
        home_kernel,
        out_shape=(jax.ShapeDtypeStruct((3,) + o.shape[1:], o.dtype), jax.ShapeDtypeStruct((3,) + s.shape[1:], s.dtype)),
        in_specs=[ANY, ANY],
        out_specs=(ANY, ANY),
        scratch_shapes=[pltpu.SemaphoreType.DMA((6,)), pltpu.SemaphoreType.DMA((6,))],
        compiler_params=pltpu.CompilerParams(collective_id=collective_id, has_side_effects=True),
        name='home_partials',
    )(o, s)


def attend_kernel(layer, n_seq, heads, scale, list_ref, q_ref, k_hbm, v_hbm, o_ref, m_out, l_out, m_acc, l_acc, kbuf, vbuf, sems):
    rows, dim = q_ref.shape[1:]
    keys = kbuf.shape[2]
    n_groups = (list_ref[3, 0] + GROUP - 1) // GROUP

    def copies(g, buf):
        out = []
        for j in range(GROUP):
            slot = list_ref[1, g * GROUP + j]
            out.append(pltpu.make_async_copy(k_hbm.at[slot, layer], kbuf.at[buf, j], sems.at[buf]))
            out.append(pltpu.make_async_copy(v_hbm.at[slot, layer], vbuf.at[buf, j], sems.at[buf]))
        return out

    for g in range(DEPTH):
        @pl.when(g < n_groups)
        def _():
            for copy in copies(g, g):
                copy.start()

    def clear(i, carry):
        o_ref[i] = jnp.zeros((rows, dim), jnp.float32)
        m_acc[i] = jnp.full((rows, dim), NEG, jnp.float32)
        l_acc[i] = jnp.zeros((rows, dim), jnp.float32)
        return carry

    lax.fori_loop(0, n_seq, clear, 0)

    row = lax.broadcasted_iota(jnp.int32, (rows, keys), 0)
    col = lax.broadcasted_iota(jnp.int32, (rows, keys), 1)
    same_head = lax.rem(col, heads) == lax.rem(row, rows // 2) // (rows // 2 // heads)
    position = jnp.where(same_head, col // heads, keys)

    def group(g, carry):
        buf = lax.rem(g, DEPTH)
        for copy in copies(g, buf):
            copy.wait()
        parts = []
        for j in range(GROUP):
            e = g * GROUP + j
            seq = list_ref[0, e]
            mask = position < list_ref[2, e]
            scores = lax.dot_general(q_ref[seq], kbuf[buf, j], (((1,), (1,)), ((), ())), preferred_element_type=jnp.float32) * scale
            scores = jnp.where(mask, scores, NEG)
            top = jnp.max(scores, axis=1, keepdims=True)
            weights = jnp.where(mask, jnp.exp(scores - top), 0.0)
            total = jnp.sum(weights, axis=1, keepdims=True)
            mixed = jnp.dot(weights.astype(jnp.bfloat16), vbuf[buf, j], preferred_element_type=jnp.float32)
            parts.append((seq, top, total, mixed))
        for seq, top, total, mixed in parts:
            top_old = m_acc[seq]
            top_new = jnp.maximum(top_old, top)
            keep = jnp.exp(top_old - top_new)
            add = jnp.exp(top - top_new)
            m_acc[seq] = top_new
            l_acc[seq] = l_acc[seq] * keep + total * add
            o_ref[seq] = o_ref[seq] * keep + mixed * add

        @pl.when(g + DEPTH < n_groups)
        def _():
            for copy in copies(g + DEPTH, buf):
                copy.start()

        return carry

    lax.fori_loop(0, n_groups, group, 0)

    lane = lax.broadcasted_iota(jnp.int32, (rows, dim), 1)
    for part in range(2):
        first = part * dim
        many = min(dim, n_seq - first)

        def pack(i, carry):
            tops, totals = carry
            here = lane == i
            return jnp.where(here, m_acc[first + i], tops), jnp.where(here, l_acc[first + i], totals)

        zero = jnp.zeros((rows, dim), jnp.float32)
        tops, totals = lax.fori_loop(0, many, pack, (zero, zero))
        m_out[:, first:first + dim] = tops
        l_out[:, first:first + dim] = totals


def attend_pages(lists, q_all, k_pool, v_pool, layer, heads, scale):
    n_seq, rows, dim = q_all.shape
    keys = k_pool.shape[2]
    return pl.pallas_call(
        functools.partial(attend_kernel, layer, n_seq, heads, scale),
        out_shape=(
            jax.ShapeDtypeStruct((n_seq, rows, dim), jnp.float32),
            jax.ShapeDtypeStruct((rows, 2 * dim), jnp.float32),
            jax.ShapeDtypeStruct((rows, 2 * dim), jnp.float32),
        ),
        in_specs=[SMEM, VMEM, ANY, ANY],
        out_specs=(VMEM, VMEM, VMEM),
        scratch_shapes=[
            pltpu.VMEM((n_seq, rows, dim), jnp.float32),
            pltpu.VMEM((n_seq, rows, dim), jnp.float32),
            pltpu.VMEM((DEPTH, GROUP, keys, dim), k_pool.dtype),
            pltpu.VMEM((DEPTH, GROUP, keys, dim), v_pool.dtype),
            pltpu.SemaphoreType.DMA((DEPTH,)),
        ],
        compiler_params=pltpu.CompilerParams(vmem_limit_bytes=48 * 1024 * 1024),
        cost_estimate=pl.CostEstimate(flops=40_000_000_000, bytes_accessed=30_000_000, transcendentals=0),
        name='attend_pages',
    )(lists, q_all, k_pool, v_pool)


def patch_kernel(n_layers, list_ref, *refs):
    rows_refs = refs[:n_layers]
    k_out, v_out, sem = refs[n_layers + 2:]
    many = list_ref[3, 0]

    def copies(i):
        row, slot, offset = list_ref[0, i], list_ref[1, i], list_ref[2, i]
        return [pltpu.make_async_copy(rows_refs[layer].at[row, kind], ref.at[slot, layer, offset], sem) for layer in range(n_layers) for kind, ref in ((0, k_out), (1, v_out))]

    def start(i, carry):
        for copy in copies(i):
            copy.start()
        return carry

    def finish(i, carry):
        for copy in copies(i):
            copy.wait()
        return carry

    lax.fori_loop(0, many, start, 0)
    lax.fori_loop(0, many, finish, 0)


def patch_pools(writes, rows, k_pool, v_pool):
    n_layers = len(rows)
    return pl.pallas_call(
        functools.partial(patch_kernel, n_layers),
        out_shape=(jax.ShapeDtypeStruct(k_pool.shape, k_pool.dtype), jax.ShapeDtypeStruct(v_pool.shape, v_pool.dtype)),
        in_specs=[SMEM] + [VMEM] * n_layers + [ANY, ANY],
        out_specs=(ANY, ANY),
        scratch_shapes=[pltpu.SemaphoreType.DMA],
        input_output_aliases={n_layers + 1: 0, n_layers + 2: 1},
        name='patch_pools',
    )(writes, *rows, k_pool, v_pool)


def move_kernel(list_ref, src_ref, *refs):
    dst_ref, ring, in_sems, out_sems = refs[-4:]
    many = list_ref[2, 0]

    def fetch(i):
        buf = lax.rem(i, RING)
        return pltpu.make_async_copy(src_ref.at[list_ref[0, i]], ring.at[buf], in_sems.at[buf])

    def store(i):
        buf = lax.rem(i, RING)
        return pltpu.make_async_copy(ring.at[buf], dst_ref.at[list_ref[1, i]], out_sems.at[buf])

    def first(i, carry):
        fetch(i).start()
        return carry

    def step(i, carry):
        fetch(i).wait()
        store(i).start()

        @pl.when(i >= LAG)
        def _():
            store(i - LAG).wait()

            @pl.when(i - LAG + RING < many)
            def _():
                fetch(i - LAG + RING).start()

        return carry

    def last(i, carry):
        store(i).wait()
        return carry

    lax.fori_loop(0, jnp.minimum(many, RING), first, 0)
    lax.fori_loop(0, many, step, 0)
    lax.fori_loop(jnp.maximum(many - LAG, 0), many, last, 0)


def move_pages(moves, src, dst):
    fresh = isinstance(dst, tuple)
    shape = dst if fresh else dst.shape
    return pl.pallas_call(
        move_kernel,
        out_shape=jax.ShapeDtypeStruct(shape, src.dtype),
        in_specs=[SMEM, ANY] if fresh else [SMEM, ANY, ANY],
        out_specs=ANY,
        scratch_shapes=[pltpu.VMEM((RING,) + src.shape[1:], src.dtype), pltpu.SemaphoreType.DMA((RING,)), pltpu.SemaphoreType.DMA((RING,))],
        input_output_aliases={} if fresh else {2: 0},
    )(*((moves, src) if fresh else (moves, src, dst)))


def compact(keep, size, *columns):
    n = keep.shape[-1]
    place = jnp.arange(n, dtype=jnp.int32)
    before = (place[:, None] < place[None, :]).astype(jnp.bfloat16)
    rank = jnp.dot(keep.astype(jnp.bfloat16), before, preferred_element_type=jnp.float32).astype(jnp.int32)
    rank = jnp.where(keep, rank, -1)
    hit = rank[:, None, :] == jnp.arange(size, dtype=jnp.int32)[None, :, None]
    packed = [jnp.sum(jnp.where(hit, column[:, None, :], 0), axis=-1) for column in columns]
    many = jnp.sum(keep.astype(jnp.int32), axis=-1)
    return jnp.stack(packed + [jnp.broadcast_to(many[:, None], packed[0].shape)], axis=1)


def solution(mesh):
    groups = mesh.shape['kv']
    rows_spec = P(None, ('rep', 'kv'), None)
    pool_spec = P(('rep', 'kv'))
    table_spec = P('rep', None)
    vec_spec = P('rep')
    full_spec = P()

    def device_fn(embeds, w_query, w_key, w_value, w_out, w_up, w_down, k_pool, v_pool, old_table, new_table, seq_len, finished, mig_src, mig_dst):
        my_dev = lax.axis_index('kv')
        slots_dev, n_layers, page_size, kv_heads, head_dim = k_pool.shape
        n_steps, seq_dev, d_model = embeds.shape
        n_batch, pages_seq = old_table.shape
        q_width = w_query.shape[2]
        kv_width = kv_heads * head_dim
        rep_factor = q_width // kv_width
        q_heads = kv_heads * rep_factor
        n_mig = mig_src.shape[0]
        scale = head_dim ** -0.5
        slot_base = my_dev * slots_dev
        last_page = pages_seq - 1
        active = finished == 0

        src_dev = mig_src // slots_dev
        dst_dev = mig_dst // slots_dev
        pair_key = src_dev * groups + dst_dev
        entry_ids = jnp.arange(n_mig, dtype=jnp.int32)
        earlier = (pair_key[None, :] == pair_key[:, None]) & (entry_ids[None, :] < entry_ids[:, None])
        pair_rank = jnp.sum(earlier.astype(jnp.int32), axis=1)
        keeps, froms, tos = [], [], []
        for pool, low, high in CHUNKS:
            wide = high - low
            ranked = (pair_rank >= low) & (pair_rank < high)
            keeps.append(ranked & (src_dev == my_dev))
            froms.append(mig_src - slot_base)
            tos.append(dst_dev * wide + pair_rank - low)
            keeps.append(ranked & (dst_dev == my_dev))
            froms.append(src_dev * wide + pair_rank - low)
            tos.append(mig_dst - slot_base)
        plan = compact(jnp.stack(keeps), slots_dev, jnp.stack(froms), jnp.stack(tos))
        pools = (k_pool, v_pool)
        received = [None] * len(CHUNKS)

        def pack(c):
            pool, low, high = CHUNKS[c]
            return move_pages(plan[2 * c], pools[pool], (groups * (high - low),) + k_pool.shape[1:])

        def send(c):
            received[c] = lax.all_to_all(pack(c), 'kv', 0, 0, tiled=True)

        for c in range(len(CHUNKS)):
            send(c)

        page_slot = old_table.reshape(-1) - slot_base
        here = (page_slot >= 0) & (page_slot < slots_dev)
        page_seq = jnp.repeat(jnp.arange(n_batch, dtype=jnp.int32), pages_seq)
        page_start = jnp.tile(jnp.arange(pages_seq, dtype=jnp.int32) * page_size, n_batch)
        page_valid = jnp.clip(jnp.repeat(seq_len, pages_seq) - page_start, 0, page_size)
        lists = compact(here[None], ENTRY_PAD, page_seq[None], page_slot[None], page_valid[None])[0]

        old_last = old_table[:, last_page]
        new_last = new_table[:, last_page]
        overwritten = jnp.any(old_last[:, None] == mig_dst[None, :], axis=1)
        moved = active & (new_last != old_last)
        seq_ids = jnp.arange(n_batch, dtype=jnp.int32)
        offset = seq_len - last_page * page_size
        write_slot = jnp.concatenate([jnp.where(overwritten, -1, old_last), jnp.where(moved, new_last, -1), jnp.where(active, new_last, -1)]) - slot_base
        write_row = jnp.concatenate([seq_ids * 2, seq_ids * 2, seq_ids * 2 + 1])
        write_offset = jnp.concatenate([offset, offset, offset + 1])
        write_here = (write_slot >= 0) & (write_slot < slots_dev)
        writes = compact(write_here[None], 2 * slots_dev, write_row[None], write_slot[None], write_offset[None])[0]

        k_pages = k_pool.reshape(slots_dev, n_layers, page_size * kv_heads, head_dim)
        v_pages = v_pool.reshape(slots_dev, n_layers, page_size * kv_heads, head_dim)
        rows = seq_dev * n_steps
        lanes = n_steps * q_heads

        def dot(a, b):
            return jnp.dot(a, b, preferred_element_type=jnp.float32)

        def split(stats):
            return stats[..., :lanes], stats[..., lanes:]

        hidden = embeds.transpose(1, 0, 2).reshape(rows, d_model)
        new_rows = []
        for layer in range(n_layers):
            query = dot(hidden, w_query[layer]).astype(jnp.bfloat16).reshape(seq_dev, lanes, head_dim)
            k_new = dot(hidden, w_key[layer]).astype(jnp.bfloat16).reshape(seq_dev, n_steps, kv_heads, head_dim)
            v_new = dot(hidden, w_value[layer]).astype(jnp.bfloat16).reshape(seq_dev, n_steps, kv_heads, head_dim)
            rows_own = jnp.stack([k_new, v_new], axis=2)

            q_all, rows_all = gather_rows([query, rows_own], 3 * layer, groups)
            q_all = q_all.reshape(n_batch, lanes, head_dim)
            new_rows.append(rows_all.reshape(n_batch * n_steps, 2, kv_heads, head_dim))
            o_part, m_part, l_part = attend_pages(lists, q_all, k_pages, v_pages, layer, kv_heads, scale)
            stats = jnp.concatenate([m_part.T[:n_batch], l_part.T[:n_batch]], axis=1).reshape(groups, seq_dev, 2 * lanes)
            o_part = o_part.reshape(groups, seq_dev, lanes, head_dim)

            o_recv, s_recv = swap_partials(o_part, stats, 3 * layer + 1)
            core = lax.rem(my_dev, 2)
            chip = my_dev // 2
            o_mine = lax.dynamic_index_in_dim(o_part.reshape(groups // 2, 2, seq_dev, lanes, head_dim), core, 1, keepdims=False)
            s_mine = lax.dynamic_index_in_dim(stats.reshape(groups // 2, 2, seq_dev, 2 * lanes), core, 1, keepdims=False)
            m_a, l_a = split(s_mine)
            m_b, l_b = split(s_recv)
            m_chip = jnp.maximum(m_a, m_b)
            f_a, f_b = jnp.exp(m_a - m_chip), jnp.exp(m_b - m_chip)
            o_chip = o_mine * f_a[..., None] + o_recv * f_b[..., None]
            s_chip = jnp.concatenate([m_chip, l_a * f_a + l_b * f_b], axis=-1)

            o_far, s_far = home_partials(o_chip, s_chip, 3 * layer + 2)
            o_near = lax.dynamic_index_in_dim(o_chip, chip, 0, keepdims=False)
            m_near, l_near = split(lax.dynamic_index_in_dim(s_chip, chip, 0, keepdims=False))
            m_far, l_far = split(s_far)
            q_own = query.astype(jnp.float32).reshape(seq_dev, n_steps, 1, kv_heads, rep_factor, head_dim)
            k_own = k_new.astype(jnp.float32).reshape(seq_dev, 1, n_steps, kv_heads, 1, head_dim)
            own = jnp.sum(q_own * k_own, axis=-1) * scale
            seen = jnp.arange(n_steps)[None, :] <= jnp.arange(n_steps)[:, None]
            own = jnp.where(seen[None, :, :, None, None], own, NEG)
            m_own = own.max(axis=2).reshape(seq_dev, lanes)
            m_all = jnp.maximum(jnp.maximum(m_near, m_far.max(axis=0)), m_own)
            p_own = jnp.exp(own - m_all.reshape(seq_dev, n_steps, 1, kv_heads, rep_factor))
            v_own = v_new.astype(jnp.float32).reshape(seq_dev, 1, n_steps, kv_heads, 1, head_dim)
            o_own = jnp.sum(p_own[..., None] * v_own, axis=2).reshape(seq_dev, lanes, head_dim)
            f_near = jnp.exp(m_near - m_all)
            f_far = jnp.exp(m_far - m_all)
            total = l_near * f_near + jnp.sum(l_far * f_far, axis=0) + jnp.sum(p_own, axis=2).reshape(seq_dev, lanes)
            o_all = o_own + o_near * f_near[..., None]
            for k in range(3):
                o_all = o_all + o_far[k] * f_far[k][..., None]
            attn = (o_all / total[..., None]).astype(jnp.bfloat16).reshape(rows, q_width)

            mixed = (hidden.astype(jnp.float32) + dot(attn, w_out[layer])).astype(jnp.bfloat16)
            inner = jax.nn.gelu(dot(mixed, w_up[layer])).astype(jnp.bfloat16)
            hidden = (mixed.astype(jnp.float32) + dot(inner, w_down[layer])).astype(jnp.bfloat16)

        slot_ids = jnp.arange(slots_dev, dtype=jnp.int32)
        every = jnp.stack([slot_ids, slot_ids, jnp.full((slots_dev,), slots_dev, jnp.int32)])
        every, takes, _ = lax.optimization_barrier((every, plan[1::2], hidden))
        outs = [move_pages(every, pool, pool.shape) for pool in pools]
        for c, (pool, low, high) in enumerate(CHUNKS):
            outs[pool] = move_pages(takes[c], received[c], outs[pool])
        k_out, v_out = patch_pools(writes, new_rows, *outs)

        home_done = lax.dynamic_slice(finished, (my_dev * seq_dev,), (seq_dev,))
        hidden = hidden.reshape(seq_dev, n_steps, d_model)
        hid_one = jnp.where(home_done[:, None] == 0, hidden[:, 1], jnp.zeros_like(hidden[:, 1]))
        return jnp.stack([hidden[:, 0], hid_one]), k_out, v_out

    in_specs = (rows_spec, full_spec, full_spec, full_spec, full_spec, full_spec, full_spec, pool_spec, pool_spec, table_spec, table_spec, vec_spec, vec_spec, vec_spec, vec_spec)

    return jax.shard_map(device_fn, mesh=mesh, in_specs=in_specs, out_specs=(rows_spec, pool_spec, pool_spec), check_vma=False)
```

```python
import functools

import jax
import jax.numpy as jnp
from jax import lax
from jax.experimental import pallas as pl
from jax.experimental.pallas import tpu as pltpu
from jax.sharding import PartitionSpec as P


MESH = pl.DeviceIdType.MESH
ANY = pl.BlockSpec(memory_space=pl.ANY)
VMEM = pl.BlockSpec(memory_space=pltpu.VMEM)
SMEM = pl.BlockSpec(memory_space=pltpu.SMEM)
NEG = -3e38
ENTRY_PAD = 160
GROUP = 4
DEPTH = 6
RING = 48
LAG = 24
CHUNKS = ((0, 0, 8), (0, 8, 18), (0, 18, 24), (1, 0, 2), (1, 2, 11), (1, 11, 24))


def peers():
    rep = lax.axis_index('rep')
    me = lax.axis_index('kv')
    core = lax.rem(me, 2)
    chip = me // 2
    x = lax.rem(chip, 2)
    y = chip // 2
    partner = me + 1 - 2 * core
    chips = (y * 2 + (1 - x), (1 - y) * 2 + x, (1 - y) * 2 + (1 - x))
    return rep, me, core, chip, partner, chips


def meet(rep, others):
    barrier = pltpu.get_barrier_semaphore()
    for other in others:
        pl.semaphore_signal(barrier, inc=1, device_id=(rep, other), device_id_type=MESH)
    pl.semaphore_wait(barrier, len(others))


def gather_kernel(many, *refs):
    x_refs, out_refs = refs[:many], refs[many:2 * many]
    local_sems, send_sems, recv_sems = refs[2 * many:]
    rep, me, core, _, partner, chips = peers()
    same = [c * 2 + core for c in chips]
    meet(rep, same + [partner])

    def remote(a, src, dst_at, k, dev):
        return pltpu.make_async_remote_copy(src_ref=src, dst_ref=out_refs[a].at[dst_at], send_sem=send_sems.at[a, k], recv_sem=recv_sems.at[a, k], device_id=(rep, dev), device_id_type=MESH)

    across = [remote(a, x_refs[a], me, k, same[k]) for a in range(many) for k in (2, 0, 1)]
    to_partner = [remote(a, x_refs[a], me, 3, partner) for a in range(many)]
    own = [pltpu.make_async_copy(x_refs[a], out_refs[a].at[me], local_sems.at[a]) for a in range(many)]
    for copy in across + to_partner + own:
        copy.start()
    forwards = []
    for a in range(many):
        for k in (2, 0, 1):
            remote(a, x_refs[a], me, k, same[k]).wait_recv()
            forward = remote(a, out_refs[a].at[same[k]], same[k], 4 + k, partner)
            forward.start()
            forwards.append(forward)
    for copy in own:
        copy.wait()
    for copy in across:
        copy.wait_send()
    for copy in to_partner + forwards:
        copy.wait()


def gather_rows(arrays, collective_id, groups):
    many = len(arrays)
    return pl.pallas_call(
        functools.partial(gather_kernel, many),
        out_shape=tuple(jax.ShapeDtypeStruct((groups,) + x.shape, x.dtype) for x in arrays),
        in_specs=[VMEM] * many,
        out_specs=(ANY,) * many,
        scratch_shapes=[pltpu.SemaphoreType.DMA((many,)), pltpu.SemaphoreType.DMA((many, 7)), pltpu.SemaphoreType.DMA((many, 7))],
        compiler_params=pltpu.CompilerParams(collective_id=collective_id, has_side_effects=True),
        name='gather_rows',
    )(*arrays)


def swap_kernel(o_ref, s_ref, o_out, s_out, send_sems, recv_sems):
    rep, _, core, _, partner, _ = peers()
    meet(rep, [partner])
    copies = []
    for c in range(4):
        theirs = c * 2 + (1 - core)
        copies.append(pltpu.make_async_remote_copy(src_ref=o_ref.at[theirs], dst_ref=o_out.at[c], send_sem=send_sems.at[c], recv_sem=recv_sems.at[c], device_id=(rep, partner), device_id_type=MESH))
        copies.append(pltpu.make_async_remote_copy(src_ref=s_ref.at[theirs], dst_ref=s_out.at[c], send_sem=send_sems.at[4 + c], recv_sem=recv_sems.at[4 + c], device_id=(rep, partner), device_id_type=MESH))
    for copy in copies:
        copy.start()
    for copy in copies:
        copy.wait()


def swap_partials(o, s, collective_id):
    return pl.pallas_call(
        swap_kernel,
        out_shape=(jax.ShapeDtypeStruct((4,) + o.shape[1:], o.dtype), jax.ShapeDtypeStruct((4,) + s.shape[1:], s.dtype)),
        in_specs=[ANY, ANY],
        out_specs=(ANY, ANY),
        scratch_shapes=[pltpu.SemaphoreType.DMA((8,)), pltpu.SemaphoreType.DMA((8,))],
        compiler_params=pltpu.CompilerParams(collective_id=collective_id, has_side_effects=True),
        name='swap_partials',
    )(o, s)


def home_kernel(o_ref, s_ref, o_out, s_out, send_sems, recv_sems):
    rep, _, core, _, _, chips = peers()
    same = [c * 2 + core for c in chips]
    meet(rep, same)
    copies = []
    for k in (2, 0, 1):
        copies.append(pltpu.make_async_remote_copy(src_ref=o_ref.at[chips[k]], dst_ref=o_out.at[k], send_sem=send_sems.at[k], recv_sem=recv_sems.at[k], device_id=(rep, same[k]), device_id_type=MESH))
        copies.append(pltpu.make_async_remote_copy(src_ref=s_ref.at[chips[k]], dst_ref=s_out.at[k], send_sem=send_sems.at[3 + k], recv_sem=recv_sems.at[3 + k], device_id=(rep, same[k]), device_id_type=MESH))
    for copy in copies:
        copy.start()
    for copy in copies:
        copy.wait()


def home_partials(o, s, collective_id):
    return pl.pallas_call(
        home_kernel,
        out_shape=(jax.ShapeDtypeStruct((3,) + o.shape[1:], o.dtype), jax.ShapeDtypeStruct((3,) + s.shape[1:], s.dtype)),
        in_specs=[ANY, ANY],
        out_specs=(ANY, ANY),
        scratch_shapes=[pltpu.SemaphoreType.DMA((6,)), pltpu.SemaphoreType.DMA((6,))],
        compiler_params=pltpu.CompilerParams(collective_id=collective_id, has_side_effects=True),
        name='home_partials',
    )(o, s)


def attend_kernel(layer, n_seq, heads, scale, list_ref, q_ref, k_hbm, v_hbm, o_ref, m_out, l_out, m_acc, l_acc, kbuf, vbuf, sems):
    rows, dim = q_ref.shape[1:]
    keys = kbuf.shape[2]
    n_groups = (list_ref[3, 0] + GROUP - 1) // GROUP

    def copies(g, buf):
        out = []
        for j in range(GROUP):
            slot = list_ref[1, g * GROUP + j]
            out.append(pltpu.make_async_copy(k_hbm.at[slot, layer], kbuf.at[buf, j], sems.at[buf]))
            out.append(pltpu.make_async_copy(v_hbm.at[slot, layer], vbuf.at[buf, j], sems.at[buf]))
        return out

    for g in range(DEPTH):
        @pl.when(g < n_groups)
        def _():
            for copy in copies(g, g):
                copy.start()

    def clear(i, carry):
        o_ref[i] = jnp.zeros((rows, dim), jnp.float32)
        m_acc[i] = jnp.full((rows, dim), NEG, jnp.float32)
        l_acc[i] = jnp.zeros((rows, dim), jnp.float32)
        return carry

    lax.fori_loop(0, n_seq, clear, 0)

    row = lax.broadcasted_iota(jnp.int32, (rows, keys), 0)
    col = lax.broadcasted_iota(jnp.int32, (rows, keys), 1)
    same_head = lax.rem(col, heads) == lax.rem(row, rows // 2) // (rows // 2 // heads)
    position = jnp.where(same_head, col // heads, keys)

    def group(g, carry):
        buf = lax.rem(g, DEPTH)
        for copy in copies(g, buf):
            copy.wait()
        parts = []
        for j in range(GROUP):
            e = g * GROUP + j
            seq = list_ref[0, e]
            mask = position < list_ref[2, e]
            scores = lax.dot_general(q_ref[seq], kbuf[buf, j], (((1,), (1,)), ((), ())), preferred_element_type=jnp.float32) * scale
            scores = jnp.where(mask, scores, NEG)
            top = jnp.max(scores, axis=1, keepdims=True)
            weights = jnp.where(mask, jnp.exp(scores - top), 0.0)
            total = jnp.sum(weights, axis=1, keepdims=True)
            mixed = jnp.dot(weights.astype(jnp.bfloat16), vbuf[buf, j], preferred_element_type=jnp.float32)
            parts.append((seq, top, total, mixed))
        for seq, top, total, mixed in parts:
            top_old = m_acc[seq]
            top_new = jnp.maximum(top_old, top)
            keep = jnp.exp(top_old - top_new)
            add = jnp.exp(top - top_new)
            m_acc[seq] = top_new
            l_acc[seq] = l_acc[seq] * keep + total * add
            o_ref[seq] = o_ref[seq] * keep + mixed * add

        @pl.when(g + DEPTH < n_groups)
        def _():
            for copy in copies(g + DEPTH, buf):
                copy.start()

        return carry

    lax.fori_loop(0, n_groups, group, 0)

    lane = lax.broadcasted_iota(jnp.int32, (rows, dim), 1)
    for part in range(2):
        first = part * dim
        many = min(dim, n_seq - first)

        def pack(i, carry):
            tops, totals = carry
            here = lane == i
            return jnp.where(here, m_acc[first + i], tops), jnp.where(here, l_acc[first + i], totals)

        zero = jnp.zeros((rows, dim), jnp.float32)
        tops, totals = lax.fori_loop(0, many, pack, (zero, zero))
        m_out[:, first:first + dim] = tops
        l_out[:, first:first + dim] = totals


def attend_pages(lists, q_all, k_pool, v_pool, layer, heads, scale):
    n_seq, rows, dim = q_all.shape
    keys = k_pool.shape[2]
    return pl.pallas_call(
        functools.partial(attend_kernel, layer, n_seq, heads, scale),
        out_shape=(
            jax.ShapeDtypeStruct((n_seq, rows, dim), jnp.float32),
            jax.ShapeDtypeStruct((rows, 2 * dim), jnp.float32),
            jax.ShapeDtypeStruct((rows, 2 * dim), jnp.float32),
        ),
        in_specs=[SMEM, VMEM, ANY, ANY],
        out_specs=(VMEM, VMEM, VMEM),
        scratch_shapes=[
            pltpu.VMEM((n_seq, rows, dim), jnp.float32),
            pltpu.VMEM((n_seq, rows, dim), jnp.float32),
            pltpu.VMEM((DEPTH, GROUP, keys, dim), k_pool.dtype),
            pltpu.VMEM((DEPTH, GROUP, keys, dim), v_pool.dtype),
            pltpu.SemaphoreType.DMA((DEPTH,)),
        ],
        compiler_params=pltpu.CompilerParams(vmem_limit_bytes=48 * 1024 * 1024),
        cost_estimate=pl.CostEstimate(flops=40_000_000_000, bytes_accessed=30_000_000, transcendentals=0),
        name='attend_pages',
    )(lists, q_all, k_pool, v_pool)


def patch_kernel(n_layers, list_ref, *refs):
    rows_refs = refs[:2 * n_layers]
    k_out, v_out, sem = refs[2 * n_layers + 2:]
    many = list_ref[3, 0]

    def copies(i):
        row, slot, offset = list_ref[0, i], list_ref[1, i], list_ref[2, i]
        return [pltpu.make_async_copy(rows_refs[kind * n_layers + layer].at[row], ref.at[slot, layer, offset], sem) for layer in range(n_layers) for kind, ref in ((0, k_out), (1, v_out))]

    def start(i, carry):
        for copy in copies(i):
            copy.start()
        return carry

    def finish(i, carry):
        for copy in copies(i):
            copy.wait()
        return carry

    lax.fori_loop(0, many, start, 0)
    lax.fori_loop(0, many, finish, 0)


def patch_pools(writes, rows, k_pool, v_pool):
    n_layers = len(rows) // 2
    return pl.pallas_call(
        functools.partial(patch_kernel, n_layers),
        out_shape=(jax.ShapeDtypeStruct(k_pool.shape, k_pool.dtype), jax.ShapeDtypeStruct(v_pool.shape, v_pool.dtype)),
        in_specs=[SMEM] + [VMEM] * len(rows) + [ANY, ANY],
        out_specs=(ANY, ANY),
        scratch_shapes=[pltpu.SemaphoreType.DMA],
        input_output_aliases={len(rows) + 1: 0, len(rows) + 2: 1},
        name='patch_pools',
    )(writes, *rows, k_pool, v_pool)


def move_kernel(list_ref, src_ref, *refs):
    dst_ref, ring, in_sems, out_sems = refs[-4:]
    many = list_ref[2, 0]

    def fetch(i):
        buf = lax.rem(i, RING)
        return pltpu.make_async_copy(src_ref.at[list_ref[0, i]], ring.at[buf], in_sems.at[buf])

    def store(i):
        buf = lax.rem(i, RING)
        return pltpu.make_async_copy(ring.at[buf], dst_ref.at[list_ref[1, i]], out_sems.at[buf])

    def first(i, carry):
        fetch(i).start()
        return carry

    def step(i, carry):
        fetch(i).wait()
        store(i).start()

        @pl.when(i >= LAG)
        def _():
            store(i - LAG).wait()

            @pl.when(i - LAG + RING < many)
            def _():
                fetch(i - LAG + RING).start()

        return carry

    def last(i, carry):
        store(i).wait()
        return carry

    lax.fori_loop(0, jnp.minimum(many, RING), first, 0)
    lax.fori_loop(0, many, step, 0)
    lax.fori_loop(jnp.maximum(many - LAG, 0), many, last, 0)


def move_pages(moves, src, dst):
    fresh = isinstance(dst, tuple)
    shape = dst if fresh else dst.shape
    return pl.pallas_call(
        move_kernel,
        out_shape=jax.ShapeDtypeStruct(shape, src.dtype),
        in_specs=[SMEM, ANY] if fresh else [SMEM, ANY, ANY],
        out_specs=ANY,
        scratch_shapes=[pltpu.VMEM((RING,) + src.shape[1:], src.dtype), pltpu.SemaphoreType.DMA((RING,)), pltpu.SemaphoreType.DMA((RING,))],
        input_output_aliases={} if fresh else {2: 0},
    )(*((moves, src) if fresh else (moves, src, dst)))


def compact(keep, size, *columns):
    n = keep.shape[-1]
    place = jnp.arange(n, dtype=jnp.int32)
    before = (place[:, None] < place[None, :]).astype(jnp.bfloat16)
    rank = jnp.dot(keep.astype(jnp.bfloat16), before, preferred_element_type=jnp.float32).astype(jnp.int32)
    rank = jnp.where(keep, rank, -1)
    hit = rank[:, None, :] == jnp.arange(size, dtype=jnp.int32)[None, :, None]
    packed = [jnp.sum(jnp.where(hit, column[:, None, :], 0), axis=-1) for column in columns]
    many = jnp.sum(keep.astype(jnp.int32), axis=-1)
    return jnp.stack(packed + [jnp.broadcast_to(many[:, None], packed[0].shape)], axis=1)


def solution(mesh):
    groups = mesh.shape['kv']
    rows_spec = P(None, ('rep', 'kv'), None)
    pool_spec = P(('rep', 'kv'))
    table_spec = P('rep', None)
    vec_spec = P('rep')
    full_spec = P()

    def device_fn(embeds, w_query, w_key, w_value, w_out, w_up, w_down, k_pool, v_pool, old_table, new_table, seq_len, finished, mig_src, mig_dst):
        my_dev = lax.axis_index('kv')
        slots_dev, n_layers, page_size, kv_heads, head_dim = k_pool.shape
        n_steps, seq_dev, d_model = embeds.shape
        n_batch, pages_seq = old_table.shape
        q_width = w_query.shape[2]
        kv_width = kv_heads * head_dim
        rep_factor = q_width // kv_width
        q_heads = kv_heads * rep_factor
        n_mig = mig_src.shape[0]
        scale = head_dim ** -0.5
        slot_base = my_dev * slots_dev
        last_page = pages_seq - 1
        active = finished == 0

        src_dev = mig_src // slots_dev
        dst_dev = mig_dst // slots_dev
        pair_key = src_dev * groups + dst_dev
        entry_ids = jnp.arange(n_mig, dtype=jnp.int32)
        earlier = (pair_key[None, :] == pair_key[:, None]) & (entry_ids[None, :] < entry_ids[:, None])
        pair_rank = jnp.sum(earlier.astype(jnp.int32), axis=1)
        keeps, froms, tos = [], [], []
        for pool, low, high in CHUNKS:
            wide = high - low
            ranked = (pair_rank >= low) & (pair_rank < high)
            keeps.append(ranked & (src_dev == my_dev))
            froms.append(mig_src - slot_base)
            tos.append(dst_dev * wide + pair_rank - low)
            keeps.append(ranked & (dst_dev == my_dev))
            froms.append(src_dev * wide + pair_rank - low)
            tos.append(mig_dst - slot_base)
        plan = compact(jnp.stack(keeps), slots_dev, jnp.stack(froms), jnp.stack(tos))
        pools = (k_pool, v_pool)
        received = [None] * len(CHUNKS)

        def pack(c):
            pool, low, high = CHUNKS[c]
            return move_pages(plan[2 * c], pools[pool], (groups * (high - low),) + k_pool.shape[1:])

        def send(c):
            received[c] = lax.all_to_all(pack(c), 'kv', 0, 0, tiled=True)

        for c in range(len(CHUNKS)):
            send(c)

        page_slot = old_table.reshape(-1) - slot_base
        here = (page_slot >= 0) & (page_slot < slots_dev)
        page_seq = jnp.repeat(jnp.arange(n_batch, dtype=jnp.int32), pages_seq)
        page_start = jnp.tile(jnp.arange(pages_seq, dtype=jnp.int32) * page_size, n_batch)
        page_valid = jnp.clip(jnp.repeat(seq_len, pages_seq) - page_start, 0, page_size)
        lists = compact(here[None], ENTRY_PAD, page_seq[None], page_slot[None], page_valid[None])[0]

        old_last = old_table[:, last_page]
        new_last = new_table[:, last_page]
        overwritten = jnp.any(old_last[:, None] == mig_dst[None, :], axis=1)
        moved = active & (new_last != old_last)
        seq_ids = jnp.arange(n_batch, dtype=jnp.int32)
        offset = seq_len - last_page * page_size
        write_slot = jnp.concatenate([jnp.where(overwritten, -1, old_last), jnp.where(moved, new_last, -1), jnp.where(active, new_last, -1)]) - slot_base
        write_row = jnp.concatenate([seq_ids * 2, seq_ids * 2, seq_ids * 2 + 1])
        write_offset = jnp.concatenate([offset, offset, offset + 1])
        write_here = (write_slot >= 0) & (write_slot < slots_dev)
        writes = compact(write_here[None], 2 * slots_dev, write_row[None], write_slot[None], write_offset[None])[0]

        k_pages = k_pool.reshape(slots_dev, n_layers, page_size * kv_heads, head_dim)
        v_pages = v_pool.reshape(slots_dev, n_layers, page_size * kv_heads, head_dim)
        rows = seq_dev * n_steps
        lanes = n_steps * q_heads

        def dot(a, b):
            return jnp.dot(a, b, preferred_element_type=jnp.float32)

        def split(stats):
            return stats[..., :lanes], stats[..., lanes:]

        hidden = embeds.transpose(1, 0, 2).reshape(rows, d_model)
        k_rows, v_rows = [], []
        for layer in range(n_layers):
            hidden_all, = gather_rows([hidden], 3 * layer, groups)
            hidden_all = hidden_all.reshape(groups * rows, d_model)
            q_all = dot(hidden_all, w_query[layer]).astype(jnp.bfloat16).reshape(n_batch, lanes, head_dim)
            k_rows.append(dot(hidden_all, w_key[layer]).astype(jnp.bfloat16).reshape(n_batch * n_steps, kv_heads, head_dim))
            v_rows.append(dot(hidden_all, w_value[layer]).astype(jnp.bfloat16).reshape(n_batch * n_steps, kv_heads, head_dim))

            def mine(values, many):
                return lax.dynamic_slice_in_dim(values, my_dev * many, many)

            query = mine(q_all, seq_dev)
            k_new = mine(k_rows[layer], rows)
            v_new = mine(v_rows[layer], rows)
            o_part, m_part, l_part = attend_pages(lists, q_all, k_pages, v_pages, layer, kv_heads, scale)
            stats = jnp.concatenate([m_part.T[:n_batch], l_part.T[:n_batch]], axis=1).reshape(groups, seq_dev, 2 * lanes)
            o_part = o_part.reshape(groups, seq_dev, lanes, head_dim)

            o_recv, s_recv = swap_partials(o_part, stats, 3 * layer + 1)
            core = lax.rem(my_dev, 2)
            chip = my_dev // 2
            o_mine = lax.dynamic_index_in_dim(o_part.reshape(groups // 2, 2, seq_dev, lanes, head_dim), core, 1, keepdims=False)
            s_mine = lax.dynamic_index_in_dim(stats.reshape(groups // 2, 2, seq_dev, 2 * lanes), core, 1, keepdims=False)
            m_a, l_a = split(s_mine)
            m_b, l_b = split(s_recv)
            m_chip = jnp.maximum(m_a, m_b)
            f_a, f_b = jnp.exp(m_a - m_chip), jnp.exp(m_b - m_chip)
            o_chip = o_mine * f_a[..., None] + o_recv * f_b[..., None]
            s_chip = jnp.concatenate([m_chip, l_a * f_a + l_b * f_b], axis=-1)

            o_far, s_far = home_partials(o_chip, s_chip, 3 * layer + 2)
            o_near = lax.dynamic_index_in_dim(o_chip, chip, 0, keepdims=False)
            m_near, l_near = split(lax.dynamic_index_in_dim(s_chip, chip, 0, keepdims=False))
            m_far, l_far = split(s_far)
            q_own = query.astype(jnp.float32).reshape(seq_dev, n_steps, 1, kv_heads, rep_factor, head_dim)
            k_own = k_new.astype(jnp.float32).reshape(seq_dev, 1, n_steps, kv_heads, 1, head_dim)
            own = jnp.sum(q_own * k_own, axis=-1) * scale
            seen = jnp.arange(n_steps)[None, :] <= jnp.arange(n_steps)[:, None]
            own = jnp.where(seen[None, :, :, None, None], own, NEG)
            m_own = own.max(axis=2).reshape(seq_dev, lanes)
            m_all = jnp.maximum(jnp.maximum(m_near, m_far.max(axis=0)), m_own)
            p_own = jnp.exp(own - m_all.reshape(seq_dev, n_steps, 1, kv_heads, rep_factor))
            v_own = v_new.astype(jnp.float32).reshape(seq_dev, 1, n_steps, kv_heads, 1, head_dim)
            o_own = jnp.sum(p_own[..., None] * v_own, axis=2).reshape(seq_dev, lanes, head_dim)
            f_near = jnp.exp(m_near - m_all)
            f_far = jnp.exp(m_far - m_all)
            total = l_near * f_near + jnp.sum(l_far * f_far, axis=0) + jnp.sum(p_own, axis=2).reshape(seq_dev, lanes)
            o_all = o_own + o_near * f_near[..., None]
            for k in range(3):
                o_all = o_all + o_far[k] * f_far[k][..., None]
            attn = (o_all / total[..., None]).astype(jnp.bfloat16).reshape(rows, q_width)

            mixed = (hidden.astype(jnp.float32) + dot(attn, w_out[layer])).astype(jnp.bfloat16)
            inner = jax.nn.gelu(dot(mixed, w_up[layer])).astype(jnp.bfloat16)
            hidden = (mixed.astype(jnp.float32) + dot(inner, w_down[layer])).astype(jnp.bfloat16)

        slot_ids = jnp.arange(slots_dev, dtype=jnp.int32)
        every = jnp.stack([slot_ids, slot_ids, jnp.full((slots_dev,), slots_dev, jnp.int32)])
        outs = [move_pages(every, pool, pool.shape) for pool in pools]
        for c, (pool, low, high) in enumerate(CHUNKS):
            outs[pool] = move_pages(plan[2 * c + 1], received[c], outs[pool])
        k_out, v_out = patch_pools(writes, k_rows + v_rows, *outs)

        home_done = lax.dynamic_slice(finished, (my_dev * seq_dev,), (seq_dev,))
        hidden = hidden.reshape(seq_dev, n_steps, d_model)
        hid_one = jnp.where(home_done[:, None] == 0, hidden[:, 1], jnp.zeros_like(hidden[:, 1]))
        return jnp.stack([hidden[:, 0], hid_one]), k_out, v_out

    in_specs = (rows_spec, full_spec, full_spec, full_spec, full_spec, full_spec, full_spec, pool_spec, pool_spec, table_spec, table_spec, vec_spec, vec_spec, vec_spec, vec_spec)

    return jax.shard_map(device_fn, mesh=mesh, in_specs=in_specs, out_specs=(rows_spec, pool_spec, pool_spec), check_vma=False)
```
